128 devices in a mesh: gx: 4 (over z), gy: 32 (over y, x, core).
Axes of the slice: x: 4, y: 4, z: 4, core: 2. Of those that a mesh axis runs over, the one named last changes fastest.
Arguments:
- tokens: bfloat16 [8192, 6144], P('gy', 'gx'), may hold values from -7.5 to 7.5, as said below
- norm_gain: float32 [6144], P('gx'), may hold values from 0.1 to 1.9
- joined_weight: bfloat16 [6144, 43008], P('gx', 'gy'), may hold values from -0.078125 to 0.078125
Outputs:
- projected: bfloat16 [256, 32, 43008], P('gx', None, 'gy')
The draws below stay inside these ranges and needn't reach their ends.
Inputs may be any that keep to these rules, and one draw needn't show every extreme that they name: Every entry of tokens lies between -7.5 and 7.5; each token's features are noise plus an offset of its own plus a slope of its own times a ramp from -1 to 1 over the 6144 features.
All inputs are finite; a program needn't handle non-finite values.
Results may differ from the reference program's by a relative error of at most 0.014.
Values may be sent and summed in bfloat16 or wider, within the bound.
A program may use at most 128 MiB of HBM per device.

```python
import jax
import jax.numpy as jnp
from jax import lax

D = 6144
F = 43008
TOK_DEV = 256
TOKENS = 8192
N_GX = 4
N_GY = 32


def draw_tokens(key, part):
    noise_key = jax.random.fold_in(key, 11)
    offset_key = jax.random.fold_in(key, 12)
    slope_key = jax.random.fold_in(key, 13)
    noise = jnp.clip(jax.random.normal(noise_key, (TOKENS, D), jnp.float32), -4.0, 4.0)
    offset = jnp.clip(0.5 * jax.random.normal(offset_key, (TOKENS, 1), jnp.float32), -2.0, 2.0)
    slope = jax.random.uniform(slope_key, (TOKENS, 1), jnp.float32, -1.5, 1.5)
    ramp = (2.0 * jnp.arange(D, dtype=jnp.float32) + 1.0) / D - 1.0
    values = noise + offset + slope * ramp[None, :]
    return jnp.clip(values, -7.5, 7.5).astype(jnp.bfloat16)


def block_levels(key, shape, pieces, low, largest):
    def one(axis_at, shards_of):
        draws = jax.random.uniform(jax.random.fold_in(jax.random.fold_in(key, 6), axis_at), (shards_of,), jnp.float32, low / len(pieces), largest / len(pieces))
        return jnp.repeat(jnp.exp(draws), shape[axis_at] // shards_of).reshape((-1,) + (1,) * (len(shape) - axis_at - 1))

    level = one(*pieces[0])
    for cut in pieces[1:]:
        level = level * one(*cut)
    return level


def bell_draw(key, extent, spread, bound, shards=(), held_as=jnp.bfloat16):
    values = spread * jax.random.normal(key, extent, jnp.float32)
    if shards:
        values = values * block_levels(key, extent, shards, -0.22, 0.18)
    return jnp.clip(values, -bound, bound).astype(held_as)


def setup_inputs(seed: int = 0) -> dict:
    key_of = jax.random.split(jax.random.key(seed), 4)
    return {
        "tokens": draw_tokens(jax.random.fold_in(key_of[3], 71), 0),
        "norm_gain": jnp.clip(1.0 + 0.18 * jax.random.normal(key_of[1], (D,), jnp.float32), 0.1, 1.9),
        "joined_weight": bell_draw(key_of[2], (D, F), D ** -0.5, 0.078125, ((0, 4), (1, 32))),
    }


epsilon = 1e-06

def reference(tokens, norm_gain, joined_weight):
    values = tokens.astype(jnp.float32)
    mean = lax.optimization_barrier(jnp.sum(values, axis=1, keepdims=True)) / D
    centered = values - mean
    variance = lax.optimization_barrier(jnp.sum(centered * centered, axis=1, keepdims=True)) / D
    normed = (centered * lax.rsqrt(variance + epsilon) * norm_gain).astype(jnp.bfloat16)
    block_width = D // N_GX
    total = jnp.zeros((normed.shape[0], joined_weight.shape[1]), jnp.float32)
    for block in range(N_GX):
        lower = block * block_width
        term = jnp.dot(normed[:, lower:lower + block_width], joined_weight[lower:lower + block_width, :], preferred_element_type=jnp.float32)
        rounded = lax.optimization_barrier(term.astype(jnp.bfloat16))
        total = total + rounded.astype(jnp.float32)
    whole = total.astype(jnp.bfloat16)
    return jnp.transpose(whole.reshape(N_GY, TOK_DEV, whole.shape[1]), (1, 0, 2))
```

```python
import functools

import jax
import jax.numpy as jnp
from jax import lax
from jax.experimental import pallas as pl
from jax.experimental.pallas import tpu as pltpu
from jax.sharding import PartitionSpec as P

epsilon = 1e-06
MESH = pl.DeviceIdType.MESH
F32 = jnp.float32
BF16 = jnp.bfloat16

PC = 256
NC = 4
T = 64
ROWS = 32 * T
QR = ROWS // 4
HR = 256
JPOS = {0: 0, 1: 1, 3: 2, 2: 3}


def kernel(
    tok_hbm, gain_hbm, w_hbm, out_hbm,
    raw, praw, gain, st_loc, st_in, TA, TB, TC, wP, wF, wG, pbuf, inbuf, facc, fF, fO,
    lsem, start_send, start_recv, w_send, w_recv, p_send, p_recv, g_send, g_recv, out_sem,
):
    depth = raw.shape[1]
    width = 4 * depth
    z = lax.axis_index("gx")
    g = lax.axis_index("gy")
    core = g % 2
    x = (g // 2) % 4
    y = g // 8
    a = x + core * (y - x)
    b = y + core * (x - y)

    def gid(a_, b_, core_):
        x_ = a_ + core_ * (b_ - a_)
        y_ = b_ + core_ * (a_ - b_)
        return (y_ * 4 + x_) * 2 + core_

    zw = z + 1 - 2 * (z % 2)
    zp = 3 - z
    zo = (z + 2) % 4
    own = z % 2
    other = 1 - own
    dev_w = (zw, g)
    dev_p = (zp, g)
    dev_o = (zo, g)
    dev_ap = (z, gid((a + 1) % 4, b, core))
    dev_am = (z, gid((a + 3) % 4, b, core))
    dev_bp = (z, gid(a, (b + 1) % 4, core))
    dev_bm = (z, gid(a, (b + 3) % 4, core))
    dev_s = (z, g + 1 - 2 * core)

    loads = [
        pltpu.make_async_copy(tok_hbm, raw, lsem.at[0]),
        pltpu.make_async_copy(gain_hbm, gain.at[own], lsem.at[1]),
    ]
    for c in range(NC):
        loads.append(pltpu.make_async_copy(w_hbm.at[:, c * PC : (c + 1) * PC], wP.at[c, own], lsem.at[2 + c]))
    loads.append(pltpu.make_async_copy(w_hbm.at[:, NC * PC :], wF.at[own], lsem.at[2 + NC]))
    for copy in loads:
        copy.start()

    barrier = pltpu.get_barrier_semaphore()
    everyone = (dev_w, dev_p, dev_o, dev_ap, dev_am, dev_bp, dev_bm, dev_s)
    for dev in everyone:
        pl.semaphore_signal(barrier, inc=1, device_id=dev, device_id_type=MESH)
    pl.semaphore_wait(barrier, len(everyone))

    sends = []

    def remote(src, dst, send, recv, dev, static=True):
        copy = pltpu.make_async_remote_copy(
            src_ref=src, dst_ref=dst, send_sem=send, recv_sem=recv, device_id=dev, device_id_type=MESH
        )
        copy.start()
        if static:
            sends.append(copy)
        return copy

    def arrived(dst, recv, dev):
        pltpu.make_async_remote_copy(
            src_ref=dst, dst_ref=dst, send_sem=recv, recv_sem=recv, device_id=dev, device_id_type=MESH
        ).wait_recv()

    def rows(start, count):
        return pl.ds(pl.multiple_of(start, count), count)

    for k, pos in enumerate((zo, zw)):
        remote(tok_hbm.at[rows(pos * T, T)], praw.at[k * T : (k + 1) * T], start_send.at[k], start_recv.at[k], dev_w)
    remote(gain_hbm, gain.at[own], start_send.at[2], start_recv.at[2], dev_w)

    loads[0].wait()

    def stats(r, carry):
        at = rows(r * T, T)
        v = raw[at, :].astype(F32)
        m = jnp.sum(v, axis=1, keepdims=True) / depth
        d = v - m
        s = jnp.sum(d * d, axis=1, keepdims=True)
        lane = lax.broadcasted_iota(jnp.int32, (T, 128), 1)
        st_loc[at, :] = jnp.where(lane < 64, m, s)
        return carry

    lax.fori_loop(0, 4, stats, 0)
    for k, (dev, first, second) in enumerate(((dev_p, z, zp), (dev_w, zo, zw), (dev_o, zw, zo))):
        for h, pos in enumerate((first, second)):
            n = 3 + 2 * k + h
            remote(st_loc.at[rows(pos * T, T)], st_in.at[k, h * T : (h + 1) * T], start_send.at[n], start_recv.at[n], dev)

    remote(w_hbm.at[:, NC * PC :], wG.at[own], w_send.at[NC], w_recv.at[NC], dev_p)
    for c in range(NC):
        remote(w_hbm.at[:, c * PC : (c + 1) * PC], wP.at[c, own], w_send.at[c], w_recv.at[c], dev_w)
    remote(w_hbm.at[:, NC * PC :], wF.at[own], w_send.at[NC + 1], w_recv.at[NC + 1], dev_w)

    loads[1].wait()
    for n in range(3, 9):
        k, h = (n - 3) // 2, (n - 3) % 2
        arrived(st_in.at[k, h * T : (h + 1) * T], start_recv.at[n], (dev_p, dev_w, dev_o)[k])
    arrived(gain.at[other], start_recv.at[2], dev_w)
    for k in range(2):
        arrived(praw.at[k * T : (k + 1) * T], start_recv.at[k], dev_w)

    for h, (dst, pos) in enumerate(((TA, zp), (TB, z))):
        parts = [st_loc[rows(pos * T, T), :]] + [st_in[k, h * T : (h + 1) * T, :] for k in range(3)]
        means = [p[:, 0:1] for p in parts]
        mean = (means[0] + means[1] + means[2] + means[3]) * 0.25
        second = jnp.zeros_like(mean)
        for p, m in zip(parts, means):
            second = second + p[:, 64:65] + depth * (m - mean) * (m - mean)
        scale = lax.rsqrt(second / width + epsilon)
        dst[own, 0:T, :] = ((raw[rows(pos * T, T), :].astype(F32) - mean) * scale * gain[own]).astype(BF16)
        dst[other, 0:T, :] = ((praw[h * T : (h + 1) * T, :].astype(F32) - mean) * scale * gain[other]).astype(BF16)

    class Gather:
        def __init__(self, k, buf):
            self.k, self.buf, self.count = k, buf, 0

        def piece(self, i, j, sib=0):
            r = JPOS[j % 4] * 8 + sib * 4 + i % 4
            return self.buf.at[:, r * T : (r + 1) * T, :]

        def slot(self, i, s):
            r = i % 4
            return self.buf.at[s, r * T : (r + 1) * T, :]

        def rsem(self, i, j, sib=0):
            return g_recv.at[self.k * 32 + sib * 16 + (j % 4) * 4 + i % 4]

        def ssem(self):
            self.count += 1
            return g_send.at[self.k * 36 + self.count - 1]

        def send(self, i, j, di, dj, dev):
            remote(self.piece(i, j), self.piece(i - di, j - dj), self.ssem(), self.rsem(i - di, j - dj), dev)

        def send_sib(self, i, j):
            remote(self.piece(i, j), self.piece(i, j, 1), self.ssem(), self.rsem(i, j, 1), dev_s)

        def send_slot(self, i, di, s, dev):
            remote(self.slot(i, s), self.slot(i - di, s), self.ssem(), g_recv.at[self.k * 32 + (2, 0)[s]], dev)

        def wait(self, i, j, dev, sib=0):
            arrived(self.piece(i, j, sib), self.rsem(i, j, sib), dev)

        def spread(self, i):
            self.send(i, 0, 0, 1, dev_bp)
            self.send(i, 0, 0, -1, dev_bm)
            self.send_sib(i, 0)

        def e1(self):
            self.send(0, 0, 1, 0, dev_ap)
            self.send(0, 0, -1, 0, dev_am)
            self.spread(0)

        def e2(self):
            self.wait(3, 0, dev_am)
            self.send_slot(3, 1, 0, dev_ap)
            self.spread(3)

        def e3(self):
            self.wait(1, 0, dev_ap)
            self.send_slot(1, -1, 1, dev_am)
            self.spread(1)

        def e4(self):
            for s, dev in ((0, dev_am), (1, dev_ap)):
                arrived(self.slot(2, s), g_recv.at[self.k * 32 + (2, 0)[s]], dev)
            self.spread(2)

        def e5(self, i):
            self.wait(i, 3, dev_bm)
            if i in (0, 1):
                self.send(i, 3, 0, 1, dev_bp)
            self.wait(i, 1, dev_bp)
            if i in (3, 2):
                self.send(i, 1, 0, -1, dev_bm)
            self.send_sib(i, 3)
            self.send_sib(i, 1)

        def e6(self):
            for i in (0, 3, 1, 2):
                self.wait(i, 2, dev_bm if i in (0, 1) else dev_bp)
                self.send_sib(i, 2)

        def e7(self, q):
            j = (0, 1, 3, 2)[q]
            for i in range(4):
                self.wait(i, j, dev_s, 1)

    A, B, C = Gather(0, TA), Gather(1, TB), Gather(2, TC)

    def own_cols(c):
        loads[2 + c].wait()
        arrived(wP.at[c, other], w_recv.at[c], dev_w)

    def pair_dot(buf, c, at):
        return jnp.dot(buf[0, at, :], wP[c, 0], preferred_element_type=F32) + jnp.dot(
            buf[1, at, :], wP[c, 1], preferred_element_type=F32
        )

    def part_copy(u):
        c, q = u // 4, u % 4
        ref = pbuf.at[c, rows(q * QR, QR)]
        dst = inbuf.at[c, rows(q * QR, QR)]
        return pltpu.make_async_remote_copy(
            src_ref=ref, dst_ref=dst, send_sem=p_send.at[u], recv_sem=p_recv.at[u], device_id=dev_p, device_id_type=MESH
        )

    def partial(lo, hi):
        def unit(u, carry):
            c, q = u // 4, u % 4

            def half(h, carry):
                at = rows(q * QR + h * HR, HR)
                pbuf[c, at, :] = pair_dot(TA, c, at).astype(BF16)
                return carry

            lax.fori_loop(0, QR // HR, half, 0)
            part_copy(u).start()
            return carry

        lax.fori_loop(lo, hi, unit, 0)

    def place(q, s):
        j = q + (q // 2) * (1 - 2 * (q % 2))
        spots = []
        for i in range(4):
            if s == 0:
                spots.append(gid((a + i) % 4, (b + j) % 4, core))
            else:
                spots.append(gid((b + i) % 4, (a + j) % 4, 1 - core))
        return spots

    def out_wait(u):
        c, q = u // 4, u % 4
        ref = inbuf.at[c, rows(q * QR, QR)]
        return pltpu.make_async_copy(ref, ref, out_sem.at[u])

    def final(lo, hi):
        def unit(u, carry):
            c, q = u // 4, u % 4

            def half(h, carry):
                facc[rows(h * HR, HR), :] = pair_dot(TB, c, rows(q * QR + h * HR, HR))
                return carry

            lax.fori_loop(0, QR // HR, half, 0)
            part_copy(u).wait_recv()
            at = rows(q * QR, QR)
            inbuf[c, at, :] = (facc[...] + inbuf[c, at, :].astype(F32)).astype(BF16)
            for s in range(2):
                for i, p in enumerate(place(q, s)):
                    pltpu.make_async_copy(
                        inbuf.at[c, rows((q * 8 + s * 4 + i) * T, T)],
                        out_hbm.at[p, :, pl.ds(pl.multiple_of(c * PC, PC), PC)],
                        out_sem.at[u],
                    ).start()
            return carry

        lax.fori_loop(lo, hi, unit, 0)

    A.e1()
    remote(A.piece(0, 0), C.piece(0, 0), start_send.at[9], start_recv.at[9], dev_p)
    A.e2()
    A.e3()
    A.e4()
    B.e1()
    A.e5(0)
    A.e5(3)
    A.e7(0)
    own_cols(0)
    partial(0, 1)
    A.e5(1)
    A.e5(2)
    A.e7(1)
    A.e7(2)
    partial(1, 3)
    B.e2()
    B.e3()
    A.e6()
    A.e7(3)
    partial(3, 4)
    B.e4()
    B.e5(0)
    own_cols(1)
    partial(4, 8)
    arrived(C.piece(0, 0), start_recv.at[9], dev_p)
    C.e1()
    B.e5(3)
    B.e5(1)
    B.e5(2)
    arrived(wG.at[zp % 2], w_recv.at[NC], dev_p)
    remote(wG.at[zp % 2], wG.at[zp % 2], w_send.at[NC + 2], w_recv.at[NC + 2], dev_w)
    own_cols(2)
    partial(8, 12)
    C.e2()
    C.e3()
    B.e6()
    C.e4()
    for q in range(4):
        B.e7(q)
    C.e5(0)
    own_cols(3)
    partial(12, 16)
    C.e5(3)
    final(0, 3)
    C.e5(1)
    final(3, 6)
    C.e5(2)
    final(6, 8)
    C.e6()
    final(8, 10)
    for q in range(4):
        C.e7(q)

    loads[2 + NC].wait()

    def last_a(r, carry):
        at = rows(r * HR, HR)
        fF[at, :] = jnp.dot(TB[own, at, :], wF[own], preferred_element_type=F32) + jnp.dot(
            TC[zp % 2, at, :], wG[zp % 2], preferred_element_type=F32
        )
        return carry

    lax.fori_loop(0, ROWS // HR, last_a, 0)
    final(10, 14)
    arrived(wF.at[other], w_recv.at[NC + 1], dev_w)

    def last_b(r, carry):
        at = rows(r * HR, HR)
        fF[at, :] = fF[at, :] + jnp.dot(TB[other, at, :], wF[other], preferred_element_type=F32)
        return carry

    lax.fori_loop(0, ROWS // HR, last_b, 0)
    arrived(wG.at[zo % 2], w_recv.at[NC + 2], dev_w)

    def last_c(r, carry):
        at = rows(r * HR, HR)
        fO[at, :] = (fF[at, :] + jnp.dot(TC[zo % 2, at, :], wG[zo % 2], preferred_element_type=F32)).astype(BF16)
        return carry

    lax.fori_loop(0, ROWS // HR, last_c, 0)
    for q in range(4):
        for s in range(2):
            for i, p in enumerate(place(q, s)):
                r = q * 8 + s * 4 + i
                pltpu.make_async_copy(
                    fO.at[r * T : (r + 1) * T], out_hbm.at[p, :, NC * PC :], out_sem.at[4 * NC]
                ).start()
    final(14, 16)

    for copy in sends:
        copy.wait_send()

    def drain(u, carry):
        part_copy(u).wait_send()
        out_wait(u).wait()
        return carry

    lax.fori_loop(0, 4 * NC, drain, 0)
    pltpu.make_async_copy(fO, fO, out_sem.at[4 * NC]).wait()


def body(tokens, norm_gain, joined_weight):
    count, depth = tokens.shape
    columns = joined_weight.shape[1]
    rest = columns - NC * PC
    any_space = pl.BlockSpec(memory_space=pl.ANY)
    dma = pltpu.SemaphoreType.DMA
    result = pl.pallas_call(
        kernel,
        out_shape=jax.ShapeDtypeStruct((32, T, columns), BF16),
        in_specs=[any_space] * 3,
        out_specs=any_space,
        scratch_shapes=[
            pltpu.VMEM((count, depth), BF16),
            pltpu.VMEM((2 * T, depth), BF16),
            pltpu.VMEM((2, 1, depth), F32),
            pltpu.VMEM((count, 128), F32),
            pltpu.VMEM((3, 2 * T, 128), F32),
            pltpu.VMEM((2, ROWS, depth), BF16),
            pltpu.VMEM((2, ROWS, depth), BF16),
            pltpu.VMEM((2, ROWS, depth), BF16),
            pltpu.VMEM((NC, 2, depth, PC), BF16),
            pltpu.VMEM((2, depth, rest), BF16),
            pltpu.VMEM((2, depth, rest), BF16),
            pltpu.VMEM((NC, ROWS, PC), BF16),
            pltpu.VMEM((NC, ROWS, PC), BF16),
            pltpu.VMEM((QR, PC), F32),
            pltpu.VMEM((ROWS, rest), F32),
            pltpu.VMEM((ROWS, rest), BF16),
            dma((3 + NC,)),
            dma((10,)),
            dma((10,)),
            dma((NC + 3,)),
            dma((NC + 3,)),
            dma((4 * NC,)),
            dma((4 * NC,)),
            dma((3 * 36,)),
            dma((3 * 32,)),
            dma((4 * NC + 1,)),
        ],
        compiler_params=pltpu.CompilerParams(
            collective_id=0, has_side_effects=True, vmem_limit_bytes=67_000_000
        ),
    )(tokens, norm_gain.reshape(1, depth), joined_weight)
    return jnp.swapaxes(result, 0, 1)


def solution(mesh):
    return jax.shard_map(
        body,
        mesh=mesh,
        in_specs=(P("gy", "gx"), P("gx"), P("gx", "gy")),
        out_specs=P("gx", None, "gy"),
        check_vma=False,
    )
```

```python
import functools

import jax
import jax.numpy as jnp
from jax import lax
from jax.experimental import pallas as pl
from jax.experimental.pallas import tpu as pltpu
from jax.sharding import PartitionSpec as P

epsilon = 1e-06
MESH = pl.DeviceIdType.MESH
F32 = jnp.float32
BF16 = jnp.bfloat16

PC = 256
NC = 4
T = 64
ROWS = 32 * T
QR = ROWS // 4
HR = 512
JPOS = {0: 0, 1: 1, 3: 2, 2: 3}


def times(rows, columns):
    return lax.dot_general(rows, columns, (((1,), (1,)), ((), ())), preferred_element_type=F32)


def kernel(
    tok_hbm, gain_hbm, w_hbm, out_hbm,
    raw, praw, gain, gain_other, st_loc, st_in, TA, TB, TC, wP, wF, wG, pbuf, inbuf, facc, fF, fO,
    lsem, start_send, start_recv, w_send, w_recv, p_send, p_recv, g_send, g_recv, out_sem,
):
    depth = raw.shape[1]
    width = 4 * depth
    z = lax.axis_index("gx")
    g = lax.axis_index("gy")
    core = g % 2
    x = (g // 2) % 4
    y = g // 8
    a = x + core * (y - x)
    b = y + core * (x - y)

    def gid(a_, b_, core_):
        x_ = a_ + core_ * (b_ - a_)
        y_ = b_ + core_ * (a_ - b_)
        return (y_ * 4 + x_) * 2 + core_

    zw = z + 1 - 2 * (z % 2)
    zp = 3 - z
    zo = (z + 2) % 4
    own = z % 2
    other = 1 - own
    dev_w = (zw, g)
    dev_p = (zp, g)
    dev_o = (zo, g)
    dev_ap = (z, gid((a + 1) % 4, b, core))
    dev_am = (z, gid((a + 3) % 4, b, core))
    dev_bp = (z, gid(a, (b + 1) % 4, core))
    dev_bm = (z, gid(a, (b + 3) % 4, core))
    dev_s = (z, g + 1 - 2 * core)

    loads = [
        pltpu.make_async_copy(tok_hbm, raw, lsem.at[0]),
        pltpu.make_async_copy(gain_hbm, gain, lsem.at[1]),
    ]
    for c in range(NC):
        loads.append(pltpu.make_async_copy(w_hbm.at[c * PC : (c + 1) * PC], wP.at[c, own], lsem.at[2 + c]))
    loads.append(pltpu.make_async_copy(w_hbm.at[NC * PC :], wF.at[own], lsem.at[2 + NC]))
    for copy in loads:
        copy.start()

    loads[0].wait()

    def rows(start, count):
        return pl.ds(pl.multiple_of(start, count), count)

    def stats(r, carry):
        at = rows(r * T, T)
        v = raw[at, :].astype(F32)
        m = jnp.sum(v, axis=1, keepdims=True) / depth
        d = v - m
        s = jnp.sum(d * d, axis=1, keepdims=True)
        lane = lax.broadcasted_iota(jnp.int32, (T, 128), 1)
        st_loc[at, :] = jnp.where(lane < 64, m, s)
        return carry

    lax.fori_loop(0, 4, stats, 0)
    loads[1].wait()

    barrier = pltpu.get_barrier_semaphore()
    everyone = (dev_w, dev_p, dev_o, dev_ap, dev_am, dev_bp, dev_bm, dev_s)
    for dev in everyone:
        pl.semaphore_signal(barrier, inc=1, device_id=dev, device_id_type=MESH)
    pl.semaphore_wait(barrier, len(everyone))

    sends = []

    def remote(src, dst, send, recv, dev, static=True):
        copy = pltpu.make_async_remote_copy(
            src_ref=src, dst_ref=dst, send_sem=send, recv_sem=recv, device_id=dev, device_id_type=MESH
        )
        copy.start()
        if static:
            sends.append(copy)
        return copy

    def arrived(dst, recv, dev):
        pltpu.make_async_remote_copy(
            src_ref=dst, dst_ref=dst, send_sem=recv, recv_sem=recv, device_id=dev, device_id_type=MESH
        ).wait_recv()

    for k, (dev, first, second) in enumerate(((dev_p, z, zp), (dev_w, zo, zw), (dev_o, zw, zo))):
        for h, pos in enumerate((first, second)):
            n = 3 + 2 * k + h
            remote(st_loc.at[rows(pos * T, T)], st_in.at[k, h * T : (h + 1) * T], start_send.at[n], start_recv.at[n], dev)
    remote(gain_hbm, gain_other, start_send.at[2], start_recv.at[2], dev_w)
    for k, pos in enumerate((zo, zw)):
        remote(raw.at[rows(pos * T, T)], praw.at[k * T : (k + 1) * T], start_send.at[k], start_recv.at[k], dev_w)

    remote(w_hbm.at[NC * PC :], wG.at[own], w_send.at[NC], w_recv.at[NC], dev_p)

    def send_cols(c):
        remote(w_hbm.at[c * PC : (c + 1) * PC], wP.at[c, own], w_send.at[c], w_recv.at[c], dev_w)

    for c in range(NC - 1):
        send_cols(c)

    def normalise(h, dst, pos):
        for k in range(3):
            n = 3 + 2 * k + h
            arrived(st_in.at[k, h * T : (h + 1) * T], start_recv.at[n], (dev_p, dev_w, dev_o)[k])
        if h == 0:
            arrived(gain_other, start_recv.at[2], dev_w)
        parts = [st_loc[rows(pos * T, T), :]] + [st_in[k, h * T : (h + 1) * T, :] for k in range(3)]
        means = [p[:, 0:1] for p in parts]
        mean = (means[0] + means[1] + means[2] + means[3]) * 0.25
        second = jnp.zeros_like(mean)
        for p, m in zip(parts, means):
            second = second + p[:, 64:65] + depth * (m - mean) * (m - mean)
        scale = lax.rsqrt(second / width + epsilon)
        dst[own, 0:T, :] = ((raw[rows(pos * T, T), :].astype(F32) - mean) * scale * gain[...].reshape(1, depth)).astype(BF16)
        arrived(praw.at[h * T : (h + 1) * T], start_recv.at[h], dev_w)
        dst[other, 0:T, :] = (
            (praw[h * T : (h + 1) * T, :].astype(F32) - mean) * scale * gain_other[...].reshape(1, depth)
        ).astype(BF16)

    class Gather:
        def __init__(self, k, buf):
            self.k, self.buf, self.count = k, buf, 0

        def piece(self, i, j, sib=0):
            r = JPOS[j % 4] * 8 + sib * 4 + i % 4
            return self.buf.at[:, r * T : (r + 1) * T, :]

        def slot(self, i, s):
            r = i % 4
            return self.buf.at[s, r * T : (r + 1) * T, :]

        def rsem(self, i, j, sib=0):
            return g_recv.at[self.k * 32 + sib * 16 + (j % 4) * 4 + i % 4]

        def ssem(self):
            self.count += 1
            return g_send.at[self.k * 36 + self.count - 1]

        def send(self, i, j, di, dj, dev):
            remote(self.piece(i, j), self.piece(i - di, j - dj), self.ssem(), self.rsem(i - di, j - dj), dev)

        def send_sib(self, i, j):
            remote(self.piece(i, j), self.piece(i, j, 1), self.ssem(), self.rsem(i, j, 1), dev_s)

        def send_slot(self, i, di, s, dev):
            remote(self.slot(i, s), self.slot(i - di, s), self.ssem(), g_recv.at[self.k * 32 + (2, 0)[s]], dev)

        def wait(self, i, j, dev, sib=0):
            arrived(self.piece(i, j, sib), self.rsem(i, j, sib), dev)

        def spread(self, i):
            self.send(i, 0, 0, 1, dev_bp)
            self.send(i, 0, 0, -1, dev_bm)
            self.send_sib(i, 0)

        def e1(self):
            self.send(0, 0, 1, 0, dev_ap)
            self.send(0, 0, -1, 0, dev_am)
            self.spread(0)

        def e2(self):
            self.wait(3, 0, dev_am)
            self.send_slot(3, 1, 0, dev_ap)
            self.spread(3)

        def e3(self):
            self.wait(1, 0, dev_ap)
            self.send_slot(1, -1, 1, dev_am)
            self.spread(1)

        def e4(self):
            for s, dev in ((0, dev_am), (1, dev_ap)):
                arrived(self.slot(2, s), g_recv.at[self.k * 32 + (2, 0)[s]], dev)
            self.spread(2)

        def e5(self, i):
            self.wait(i, 3, dev_bm)
            if i in (0, 1):
                self.send(i, 3, 0, 1, dev_bp)
            self.wait(i, 1, dev_bp)
            if i in (3, 2):
                self.send(i, 1, 0, -1, dev_bm)
            self.send_sib(i, 3)
            self.send_sib(i, 1)

        def e6(self):
            for i in (0, 3, 1, 2):
                self.wait(i, 2, dev_bm if i in (0, 1) else dev_bp)
                self.send_sib(i, 2)

        def e7(self, q):
            j = (0, 1, 3, 2)[q]
            for i in range(4):
                self.wait(i, j, dev_s, 1)

    A, B, C = Gather(0, TA), Gather(1, TB), Gather(2, TC)

    def own_cols(c):
        loads[2 + c].wait()
        arrived(wP.at[c, other], w_recv.at[c], dev_w)

    def pair_dot(buf, c, at):
        return times(buf[0, at, :], wP[c, 0]) + times(buf[1, at, :], wP[c, 1])

    def part_copy(u):
        c, q = u // 4, u % 4
        ref = pbuf.at[c, rows(q * QR, QR)]
        dst = inbuf.at[c, rows(q * QR, QR)]
        return pltpu.make_async_remote_copy(
            src_ref=ref, dst_ref=dst, send_sem=p_send.at[u], recv_sem=p_recv.at[u], device_id=dev_p, device_id_type=MESH
        )

    def partial(lo, hi):
        def unit(u, carry):
            c, q = u // 4, u % 4

            def half(h, carry):
                at = rows(q * QR + h * HR, HR)
                pbuf[c, at, :] = pair_dot(TA, c, at).astype(BF16)
                return carry

            lax.fori_loop(0, QR // HR, half, 0)
            part_copy(u).start()
            return carry

        lax.fori_loop(lo, hi, unit, 0)

    def place(q, s):
        j = q + (q // 2) * (1 - 2 * (q % 2))
        spots = []
        for i in range(4):
            if s == 0:
                spots.append(gid((a + i) % 4, (b + j) % 4, core))
            else:
                spots.append(gid((b + i) % 4, (a + j) % 4, 1 - core))
        return spots

    def out_wait(u):
        c, q = u // 4, u % 4
        ref = inbuf.at[c, rows(q * QR, QR)]
        return pltpu.make_async_copy(ref, ref, out_sem.at[u])

    def final(lo, hi):
        def unit(u, carry):
            c, q = u // 4, u % 4

            def half(h, carry):
                facc[rows(h * HR, HR), :] = pair_dot(TB, c, rows(q * QR + h * HR, HR))
                return carry

            lax.fori_loop(0, QR // HR, half, 0)
            part_copy(u).wait_recv()
            at = rows(q * QR, QR)
            inbuf[c, at, :] = (facc[...] + inbuf[c, at, :].astype(F32)).astype(BF16)
            for s in range(2):
                for i, p in enumerate(place(q, s)):
                    pltpu.make_async_copy(
                        inbuf.at[c, rows((q * 8 + s * 4 + i) * T, T)],
                        out_hbm.at[p, :, pl.ds(pl.multiple_of(c * PC, PC), PC)],
                        out_sem.at[u],
                    ).start()
            return carry

        lax.fori_loop(lo, hi, unit, 0)

    def last_a(r, carry):
        at = rows(r * QR, QR)
        fF[at, :] = times(TB[own, at, :], wF[own]) + times(TC[zp % 2, at, :], wG[zp % 2])
        fF[at, 0:PC] = fF[at, 0:PC] + times(TC[zo % 2, at, :], wG[zo % 2, 0:PC, :])
        return carry

    def last_b(r, carry):
        at = rows(r * QR, QR)
        fF[at, :] = fF[at, :] + times(TB[other, at, :], wF[other])
        return carry

    def last_c(r, carry):
        at = rows(r * QR, QR)
        fO[at, 0:PC] = fF[at, 0:PC].astype(BF16)
        fO[at, PC:] = (fF[at, PC:] + times(TC[zo % 2, at, :], wG[zo % 2, PC:, :])).astype(BF16)
        return carry

    def forward_last(k):
        part = (slice(0, PC), slice(PC, None))[k]
        remote(wG.at[zp % 2, part], wG.at[zp % 2, part], w_send.at[NC + 2 + k], w_recv.at[NC + 2 + k], dev_w)

    normalise(0, TA, zp)
    A.e1()
    remote(A.piece(0, 0), C.piece(0, 0), start_send.at[9], start_recv.at[9], dev_p)
    normalise(1, TB, z)
    A.e2()
    A.e3()
    A.e4()
    B.e1()
    A.e5(0)
    A.e5(3)
    arrived(wG.at[zp % 2], w_recv.at[NC], dev_p)
    forward_last(0)
    send_cols(NC - 1)
    remote(w_hbm.at[NC * PC :], wF.at[own], w_send.at[NC + 1], w_recv.at[NC + 1], dev_w)
    forward_last(1)
    A.e5(1)
    A.e7(0)
    own_cols(0)
    partial(0, 1)
    A.e5(2)
    A.e7(1)
    partial(1, 2)
    A.e7(2)
    partial(2, 3)
    B.e2()
    B.e3()
    A.e6()
    A.e7(3)
    partial(3, 4)
    B.e4()
    arrived(C.piece(0, 0), start_recv.at[9], dev_p)
    C.e1()
    B.e5(0)
    own_cols(1)
    partial(4, 6)
    B.e5(3)
    partial(6, 8)
    B.e5(1)
    B.e5(2)
    C.e2()
    C.e3()
    own_cols(2)
    partial(8, 10)
    B.e6()
    C.e4()
    partial(10, 12)
    for q in range(4):
        B.e7(q)
    C.e5(0)
    final(0, 2)
    C.e5(3)
    final(2, 4)
    C.e5(1)
    final(4, 6)
    C.e5(2)
    final(6, 8)
    own_cols(3)
    partial(12, 14)
    C.e6()
    partial(14, 16)
    loads[2 + NC].wait()
    arrived(wG.at[zo % 2, 0:PC], w_recv.at[NC + 2], dev_w)
    final(8, 10)
    for q in range(4):
        C.e7(q)
        lax.fori_loop(q, q + 1, last_a, 0)
    final(10, 15)
    arrived(wF.at[other], w_recv.at[NC + 1], dev_w)
    lax.fori_loop(0, 4, last_b, 0)
    arrived(wG.at[zo % 2, PC:], w_recv.at[NC + 3], dev_w)
    lax.fori_loop(0, 4, last_c, 0)
    for q in range(4):
        for s in range(2):
            for i, p in enumerate(place(q, s)):
                r = q * 8 + s * 4 + i
                pltpu.make_async_copy(
                    fO.at[r * T : (r + 1) * T], out_hbm.at[p, :, NC * PC :], out_sem.at[4 * NC]
                ).start()
    final(15, 16)

    for copy in sends:
        copy.wait_send()

    def drain(u, carry):
        part_copy(u).wait_send()
        out_wait(u).wait()
        return carry

    lax.fori_loop(0, 4 * NC, drain, 0)
    pltpu.make_async_copy(fO, fO, out_sem.at[4 * NC]).wait()


def body(tokens, norm_gain, joined_weight):
    count, depth = tokens.shape
    columns = joined_weight.shape[1]
    rest = columns - NC * PC
    any_space = pl.BlockSpec(memory_space=pl.ANY)
    dma = pltpu.SemaphoreType.DMA
    result = pl.pallas_call(
        kernel,
        out_shape=jax.ShapeDtypeStruct((32, T, columns), BF16),
        in_specs=[any_space] * 3,
        out_specs=any_space,
        scratch_shapes=[
            pltpu.VMEM((count, depth), BF16),
            pltpu.VMEM((2 * T, depth), BF16),
            pltpu.VMEM((depth,), F32),
            pltpu.VMEM((depth,), F32),
            pltpu.VMEM((count, 128), F32),
            pltpu.VMEM((3, 2 * T, 128), F32),
            pltpu.VMEM((2, ROWS, depth), BF16),
            pltpu.VMEM((2, ROWS, depth), BF16),
            pltpu.VMEM((2, ROWS, depth), BF16),
            pltpu.VMEM((NC, 2, PC, depth), BF16),
            pltpu.VMEM((2, rest, depth), BF16),
            pltpu.VMEM((2, rest, depth), BF16),
            pltpu.VMEM((NC, ROWS, PC), BF16),
            pltpu.VMEM((NC, ROWS, PC), BF16),
            pltpu.VMEM((QR, PC), F32),
            pltpu.VMEM((ROWS, rest), F32),
            pltpu.VMEM((ROWS, rest), BF16),
            dma((3 + NC,)),
            dma((10,)),
            dma((10,)),
            dma((NC + 4,)),
            dma((NC + 4,)),
            dma((4 * NC,)),
            dma((4 * NC,)),
            dma((3 * 36,)),
            dma((3 * 32,)),
            dma((4 * NC + 1,)),
        ],
        compiler_params=pltpu.CompilerParams(
            collective_id=0, has_side_effects=True, vmem_limit_bytes=67_000_000
        ),
    )(tokens, norm_gain, joined_weight.T)
    return jnp.swapaxes(result, 0, 1)


def solution(mesh):
    return jax.shard_map(
        body,
        mesh=mesh,
        in_specs=(P("gy", "gx"), P("gx"), P("gx", "gy")),
        out_specs=P("gx", None, "gy"),
        check_vma=False,
    )
```

```python
import functools

import jax
import jax.numpy as jnp
from jax import lax
from jax.experimental import pallas as pl
from jax.experimental.pallas import tpu as pltpu
from jax.sharding import PartitionSpec as P

epsilon = 1e-06
MESH = pl.DeviceIdType.MESH
F32 = jnp.float32
BF16 = jnp.bfloat16

PC = 256
NC = 4
T = 64
ROWS = 32 * T
QR = ROWS // 4
JPOS = {0: 0, 1: 1, 3: 2, 2: 3}


def times(rows, columns):
    return lax.dot_general(rows, columns, (((1,), (1,)), ((), ())), preferred_element_type=F32)


def kernel(
    tok_hbm, gain_hbm, w_hbm, out_hbm,
    raw, praw, gain, gain_other, st_loc, st_in, TA, TB, TC, wP, wF, wG, pbuf, inbuf, facc, fF, fO,
    lsem, start_send, start_recv, w_send, w_recv, p_send, p_recv, g_send, g_recv, out_sem,
):
    depth = raw.shape[1]
    width = 4 * depth
    z = lax.axis_index("gx")
    g = lax.axis_index("gy")
    core = g % 2
    x = (g // 2) % 4
    y = g // 8
    a = x + core * (y - x)
    b = y + core * (x - y)

    def gid(a_, b_, core_):
        x_ = a_ + core_ * (b_ - a_)
        y_ = b_ + core_ * (a_ - b_)
        return (y_ * 4 + x_) * 2 + core_

    zw = z + 1 - 2 * (z % 2)
    zp = 3 - z
    zo = (z + 2) % 4
    own = z % 2
    other = 1 - own
    dev_w = (zw, g)
    dev_p = (zp, g)
    dev_o = (zo, g)
    dev_ap = (z, gid((a + 1) % 4, b, core))
    dev_am = (z, gid((a + 3) % 4, b, core))
    dev_bp = (z, gid(a, (b + 1) % 4, core))
    dev_bm = (z, gid(a, (b + 3) % 4, core))
    dev_s = (z, g + 1 - 2 * core)

    loads = [
        pltpu.make_async_copy(tok_hbm, raw, lsem.at[0]),
        pltpu.make_async_copy(gain_hbm, gain, lsem.at[1]),
    ]
    for c in range(NC):
        loads.append(pltpu.make_async_copy(w_hbm.at[c * PC : (c + 1) * PC], wP.at[c, own], lsem.at[2 + c]))
    loads.append(pltpu.make_async_copy(w_hbm.at[NC * PC :], wF.at[own], lsem.at[2 + NC]))
    for copy in loads:
        copy.start()

    lane = lax.broadcasted_iota(jnp.int32, (T, 128), 1)
    line = lax.broadcasted_iota(jnp.int32, (T, 128), 0)
    loads[0].wait()

    def rows(start, count):
        return pl.ds(start if isinstance(start, int) else pl.multiple_of(start, count), count)

    def stats(r, carry):
        at = rows(r * T, T)
        v = raw[at, :].astype(F32)
        m = jnp.sum(v, axis=1, keepdims=True) / depth
        d = v - m
        s = jnp.sum(d * d, axis=1, keepdims=True)
        both = jnp.where(lane == line, m, jnp.where(lane == line + T, s, 0.0))
        st_loc[r] = jnp.broadcast_to(jnp.sum(both, axis=0, keepdims=True), (8, 128))
        return carry

    lax.fori_loop(0, 4, stats, 0)
    loads[1].wait()

    barrier = pltpu.get_barrier_semaphore()
    everyone = (dev_w, dev_p, dev_o, dev_ap, dev_am, dev_bp, dev_bm, dev_s)
    for dev in everyone:
        pl.semaphore_signal(barrier, inc=1, device_id=dev, device_id_type=MESH)
    pl.semaphore_wait(barrier, len(everyone))

    sends = []

    def remote(src, dst, send, recv, dev, static=True):
        copy = pltpu.make_async_remote_copy(
            src_ref=src, dst_ref=dst, send_sem=send, recv_sem=recv, device_id=dev, device_id_type=MESH
        )
        copy.start()
        if static:
            sends.append(copy)
        return copy

    def arrived(dst, recv, dev):
        pltpu.make_async_remote_copy(
            src_ref=dst, dst_ref=dst, send_sem=recv, recv_sem=recv, device_id=dev, device_id_type=MESH
        ).wait_recv()

    for k, (dev, first, second) in enumerate(((dev_p, z, zp), (dev_w, zo, zw), (dev_o, zw, zo))):
        for h, pos in enumerate((first, second)):
            n = 3 + 2 * k + h
            remote(st_loc.at[pos], st_in.at[k, h], start_send.at[n], start_recv.at[n], dev)
    remote(gain_hbm, gain_other, start_send.at[2], start_recv.at[2], dev_w)
    for k, pos in enumerate((zo, zw)):
        remote(raw.at[rows(pos * T, T)], praw.at[k * T : (k + 1) * T], start_send.at[k], start_recv.at[k], dev_w)

    remote(w_hbm.at[NC * PC :], wG.at[own], w_send.at[NC], w_recv.at[NC], dev_p)

    def send_cols(c):
        remote(w_hbm.at[c * PC : (c + 1) * PC], wP.at[c, own], w_send.at[c], w_recv.at[c], dev_w)

    for c in range(NC - 1):
        send_cols(c)

    def normalise(h, dst, pos):
        for k in range(3):
            n = 3 + 2 * k + h
            arrived(st_in.at[k, h], start_recv.at[n], (dev_p, dev_w, dev_o)[k])
        if h == 0:
            arrived(gain_other, start_recv.at[2], dev_w)
        parts = [st_loc[pos]] + [st_in[k, h] for k in range(3)]
        means = [jnp.sum(jnp.where(lane == line, p[0:1, :], 0.0), axis=1, keepdims=True) for p in parts]
        seconds = [jnp.sum(jnp.where(lane == line + T, p[0:1, :], 0.0), axis=1, keepdims=True) for p in parts]
        mean = (means[0] + means[1] + means[2] + means[3]) * 0.25
        second = jnp.zeros_like(mean)
        for m, v in zip(means, seconds):
            second = second + v + depth * (m - mean) * (m - mean)
        scale = lax.rsqrt(second / width + epsilon)
        dst[own, 0:T, :] = ((raw[rows(pos * T, T), :].astype(F32) - mean) * scale * gain[...].reshape(1, depth)).astype(BF16)
        arrived(praw.at[h * T : (h + 1) * T], start_recv.at[h], dev_w)
        dst[other, 0:T, :] = (
            (praw[h * T : (h + 1) * T, :].astype(F32) - mean) * scale * gain_other[...].reshape(1, depth)
        ).astype(BF16)

    class Gather:
        def __init__(self, k, buf):
            self.k, self.buf, self.count = k, buf, 0

        def piece(self, i, j, sib=0):
            r = JPOS[j % 4] * 8 + sib * 4 + i % 4
            return self.buf.at[:, r * T : (r + 1) * T, :]

        def slot(self, i, s):
            r = i % 4
            return self.buf.at[s, r * T : (r + 1) * T, :]

        def rsem(self, i, j, sib=0):
            return g_recv.at[self.k * 32 + sib * 16 + (j % 4) * 4 + i % 4]

        def ssem(self):
            self.count += 1
            return g_send.at[self.k * 36 + self.count - 1]

        def send(self, i, j, di, dj, dev):
            remote(self.piece(i, j), self.piece(i - di, j - dj), self.ssem(), self.rsem(i - di, j - dj), dev)

        def send_sib(self, i, j):
            remote(self.piece(i, j), self.piece(i, j, 1), self.ssem(), self.rsem(i, j, 1), dev_s)

        def send_slot(self, i, di, s, dev):
            remote(self.slot(i, s), self.slot(i - di, s), self.ssem(), g_recv.at[self.k * 32 + (2, 0)[s]], dev)

        def wait(self, i, j, dev, sib=0):
            arrived(self.piece(i, j, sib), self.rsem(i, j, sib), dev)

        def spread(self, i):
            self.send(i, 0, 0, 1, dev_bp)
            self.send(i, 0, 0, -1, dev_bm)
            self.send_sib(i, 0)

        def e1(self):
            self.send(0, 0, 1, 0, dev_ap)
            self.send(0, 0, -1, 0, dev_am)
            self.spread(0)

        def e2(self):
            self.wait(3, 0, dev_am)
            self.send_slot(3, 1, 0, dev_ap)
            self.spread(3)

        def e3(self):
            self.wait(1, 0, dev_ap)
            self.send_slot(1, -1, 1, dev_am)
            self.spread(1)

        def e4(self):
            for s, dev in ((0, dev_am), (1, dev_ap)):
                arrived(self.slot(2, s), g_recv.at[self.k * 32 + (2, 0)[s]], dev)
            self.spread(2)

        def l(self, i):
            self.wait(i, 3, dev_bm)
            if i in (0, 1):
                self.send(i, 3, 0, 1, dev_bp)
            self.send_sib(i, 3)

        def r(self, i):
            self.wait(i, 1, dev_bp)
            if i in (3, 2):
                self.send(i, 1, 0, -1, dev_bm)
            self.send_sib(i, 1)

        def o(self, i):
            self.wait(i, 2, dev_bm if i in (0, 1) else dev_bp)
            self.send_sib(i, 2)

        def e7(self, q):
            j = (0, 1, 3, 2)[q]
            for i in range(4):
                self.wait(i, j, dev_s, 1)

    A, B, C = Gather(0, TA), Gather(1, TB), Gather(2, TC)

    def own_cols(c):
        loads[2 + c].wait()
        arrived(wP.at[c, other], w_recv.at[c], dev_w)

    def pair_dot(buf, c, at):
        return times(buf[0, at, :], wP[c, 0]) + times(buf[1, at, :], wP[c, 1])

    def part_copy(u):
        c, q = u // 4, u % 4
        ref = pbuf.at[c, rows(q * QR, QR)]
        dst = inbuf.at[c, rows(q * QR, QR)]
        return pltpu.make_async_remote_copy(
            src_ref=ref, dst_ref=dst, send_sem=p_send.at[u], recv_sem=p_recv.at[u], device_id=dev_p, device_id_type=MESH
        )

    def each(unit, units):
        def step(k, carry):
            u = units[0]
            for n in range(1, len(units)):
                u = jnp.where(k == n, units[n], u)
            return unit(u, carry)

        if len(units) == 1:
            unit(units[0], 0)
        else:
            lax.fori_loop(0, len(units), step, 0)

    def partial(*units):
        def unit(u, carry):
            c, q = u // 4, u % 4

            at = rows(q * QR, QR)
            pbuf[c, at, :] = pair_dot(TA, c, at).astype(BF16)
            part_copy(u).start()
            return carry

        each(unit, units)

    def place(q, s):
        j = q + (q // 2) * (1 - 2 * (q % 2))
        spots = []
        for i in range(4):
            if s == 0:
                spots.append(gid((a + i) % 4, (b + j) % 4, core))
            else:
                spots.append(gid((b + i) % 4, (a + j) % 4, 1 - core))
        return spots

    def out_wait(u):
        c, q = u // 4, u % 4
        ref = inbuf.at[c, rows(q * QR, QR)]
        return pltpu.make_async_copy(ref, ref, out_sem.at[u])

    def final(*units):
        def unit(u, carry):
            c, q = u // 4, u % 4

            at = rows(q * QR, QR)
            facc[...] = pair_dot(TB, c, at)
            part_copy(u).wait_recv()
            inbuf[c, at, :] = (facc[...] + inbuf[c, at, :].astype(F32)).astype(BF16)
            for s in range(2):
                for i, p in enumerate(place(q, s)):
                    pltpu.make_async_copy(
                        inbuf.at[c, rows((q * 8 + s * 4 + i) * T, T)],
                        out_hbm.at[p, :, rows(c * PC, PC)],
                        out_sem.at[u],
                    ).start()
            return carry

        each(unit, units)

    def last_a(r):
        at = rows(r * QR, QR)
        fF[at, :] = times(TB[own, at, :], wF[own]) + times(TC[zp % 2, at, :], wG[zp % 2])
        fF[at, 0:PC] = fF[at, 0:PC] + times(TC[zo % 2, at, :], wG[zo % 2, 0:PC, :])

    def last_b(r, carry):
        at = rows(r * QR, QR)
        fF[at, :] = fF[at, :] + times(TB[other, at, :], wF[other])
        return carry

    def last_c(r, carry):
        at = rows(r * QR, QR)
        fO[at, 0:PC] = fF[at, 0:PC].astype(BF16)
        fO[at, PC:] = (fF[at, PC:] + times(TC[zo % 2, at, :], wG[zo % 2, PC:, :])).astype(BF16)
        return carry

    def forward_last(k):
        part = (slice(0, PC), slice(PC, None))[k]
        remote(wG.at[zp % 2, part], wG.at[zp % 2, part], w_send.at[NC + 2 + k], w_recv.at[NC + 2 + k], dev_w)

    def send_last():
        arrived(wG.at[zp % 2], w_recv.at[NC], dev_p)
        forward_last(0)
        send_cols(NC - 1)
        remote(w_hbm.at[NC * PC :], wF.at[own], w_send.at[NC + 1], w_recv.at[NC + 1], dev_w)
        forward_last(1)

    def send_across():
        remote(A.piece(0, 0), C.piece(0, 0), start_send.at[9], start_recv.at[9], dev_p)

    def put_last():
        for q in range(4):
            for s in range(2):
                for i, p in enumerate(place(q, s)):
                    r = q * 8 + s * 4 + i
                    pltpu.make_async_copy(
                        fO.at[r * T : (r + 1) * T], out_hbm.at[p, :, NC * PC :], out_sem.at[4 * NC]
                    ).start()

    normalise(0, TA, zp)
    A.e1()
    send_across()
    A.e3()
    A.e2()
    A.e4()
    A.l(1)
    normalise(1, TB, z)
    send_last()
    own_cols(0)
    A.r(0)
    A.e7(0)
    A.l(0)
    A.r(3)
    partial(0)
    A.l(3)
    A.l(2)
    A.r(1)
    B.e1()
    A.e7(2)
    partial(2)
    A.r(2)
    A.e7(1)
    partial(1)
    A.o(3)
    A.o(0)
    own_cols(1)
    B.e2()
    B.r(0)
    B.e3()
    partial(6, 4, 5)
    arrived(C.piece(0, 0), start_recv.at[9], dev_p)
    A.o(1)
    B.e4()
    B.r(3)
    C.e1()
    own_cols(2)
    A.o(2)
    B.e7(0)
    A.e7(3)
    partial(8, 11)
    B.l(0)
    B.l(3)
    C.e3()
    B.l(2)
    B.l(1)
    B.r(2)
    B.r(1)
    B.e7(2)
    C.e2()
    partial(3, 9, 7, 10)
    B.e7(1)
    B.o(3)
    C.e4()
    final(6, 1, 4, 5)
    C.l(0)
    B.o(0)
    C.l(1)
    final(8, 2, 0)
    C.e7(0)
    B.o(2)
    B.o(1)
    loads[2 + NC].wait()
    arrived(wG.at[zo % 2, 0:PC], w_recv.at[NC + 2], dev_w)
    last_a(0)
    C.r(1)
    C.r(3)
    own_cols(3)
    partial(15, 13, 14, 12)
    C.r(2)
    C.l(2)
    B.e7(3)
    C.r(0)
    C.l(3)
    final(3, 9, 7, 11)
    C.o(3)
    C.o(0)
    C.e7(1)
    last_a(1)
    C.o(1)
    C.e7(2)
    last_a(2)
    C.o(2)
    final(15, 10, 13)
    C.e7(3)
    last_a(3)
    arrived(wF.at[other], w_recv.at[NC + 1], dev_w)
    lax.fori_loop(0, 4, last_b, 0)
    final(14)
    arrived(wG.at[zo % 2, PC:], w_recv.at[NC + 3], dev_w)
    lax.fori_loop(0, 4, last_c, 0)
    put_last()
    final(12)

    for copy in sends:
        copy.wait_send()

    def drain(u, carry):
        part_copy(u).wait_send()
        out_wait(u).wait()
        return carry

    lax.fori_loop(0, 4 * NC, drain, 0)
    pltpu.make_async_copy(fO, fO, out_sem.at[4 * NC]).wait()


def body(tokens, norm_gain, joined_weight):
    count, depth = tokens.shape
    columns = joined_weight.shape[1]
    rest = columns - NC * PC
    any_space = pl.BlockSpec(memory_space=pl.ANY)
    dma = pltpu.SemaphoreType.DMA
    result = pl.pallas_call(
        kernel,
        out_shape=jax.ShapeDtypeStruct((32, T, columns), BF16),
        in_specs=[any_space] * 3,
        out_specs=any_space,
        scratch_shapes=[
            pltpu.VMEM((count, depth), BF16),
            pltpu.VMEM((2 * T, depth), BF16),
            pltpu.VMEM((depth,), F32),
            pltpu.VMEM((depth,), F32),
            pltpu.VMEM((4, 8, 128), F32),
            pltpu.VMEM((3, 2, 8, 128), F32),
            pltpu.VMEM((2, ROWS, depth), BF16),
            pltpu.VMEM((2, ROWS, depth), BF16),
            pltpu.VMEM((2, ROWS, depth), BF16),
            pltpu.VMEM((NC, 2, PC, depth), BF16),
            pltpu.VMEM((2, rest, depth), BF16),
            pltpu.VMEM((2, rest, depth), BF16),
            pltpu.VMEM((NC, ROWS, PC), BF16),
            pltpu.VMEM((NC, ROWS, PC), BF16),
            pltpu.VMEM((QR, PC), F32),
            pltpu.VMEM((ROWS, rest), F32),
            pltpu.VMEM((ROWS, rest), BF16),
            dma((3 + NC,)),
            dma((10,)),
            dma((10,)),
            dma((NC + 4,)),
            dma((NC + 4,)),
            dma((4 * NC,)),
            dma((4 * NC,)),
            dma((3 * 36,)),
            dma((3 * 32,)),
            dma((4 * NC + 1,)),
        ],
        compiler_params=pltpu.CompilerParams(
            collective_id=0, has_side_effects=True, vmem_limit_bytes=67_000_000
        ),
    )(tokens, norm_gain, joined_weight.T)
    return jnp.swapaxes(result, 0, 1)


def solution(mesh):
    return jax.shard_map(
        body,
        mesh=mesh,
        in_specs=(P("gy", "gx"), P("gx"), P("gx", "gy")),
        out_specs=P("gx", None, "gy"),
        check_vma=False,
    )
```

```python
import functools

import jax
import jax.numpy as jnp
from jax import lax
from jax.experimental import pallas as pl
from jax.experimental.pallas import tpu as pltpu
from jax.sharding import PartitionSpec as P

epsilon = 1e-06
MESH = pl.DeviceIdType.MESH
F32 = jnp.float32
BF16 = jnp.bfloat16

PC = 256
NC = 4
T = 64
ROWS = 32 * T
QR = ROWS // 4
TR = T // 4
RING = 7
LIMIT = 61_000_000
JPOS = {0: 0, 1: 1, 3: 2, 2: 3}


def times(rows, columns):
    return lax.dot_general(rows, columns, (((1,), (1,)), ((), ())), preferred_element_type=F32)


def kernel(
    tok_hbm, gain_hbm, w_hbm, out,
    raw, praw, gain, gain_other, st_loc, st_in, TA, TB, TC, wP, wF, wG, pbuf, inbuf, facc, fO,
    lsem, start_send, start_recv, w_send, w_recv, p_send, p_recv, g_send, g_recv,
):
    depth = raw.shape[1]
    width = 4 * depth
    z = lax.axis_index("gx")
    g = lax.axis_index("gy")
    core = g % 2
    x = (g // 2) % 4
    y = g // 8
    a = x + core * (y - x)
    b = y + core * (x - y)

    def gid(a_, b_, core_):
        x_ = a_ + core_ * (b_ - a_)
        y_ = b_ + core_ * (a_ - b_)
        return (y_ * 4 + x_) * 2 + core_

    zw = z + 1 - 2 * (z % 2)
    zp = 3 - z
    zo = (z + 2) % 4
    own = z % 2
    other = 1 - own
    dev_w = (zw, g)
    dev_p = (zp, g)
    dev_o = (zo, g)
    dev_ap = (z, gid((a + 1) % 4, b, core))
    dev_am = (z, gid((a + 3) % 4, b, core))
    dev_bp = (z, gid(a, (b + 1) % 4, core))
    dev_bm = (z, gid(a, (b + 3) % 4, core))
    dev_s = (z, g + 1 - 2 * core)

    loads = [
        pltpu.make_async_copy(tok_hbm, raw, lsem.at[0]),
        pltpu.make_async_copy(gain_hbm, gain, lsem.at[1]),
    ]
    for c in range(NC):
        loads.append(pltpu.make_async_copy(w_hbm.at[c * PC : (c + 1) * PC], wP.at[c, own], lsem.at[2 + c]))
    loads.append(pltpu.make_async_copy(w_hbm.at[NC * PC :], wF.at[own], lsem.at[2 + NC]))
    for copy in loads:
        copy.start()

    barrier = pltpu.get_barrier_semaphore()
    everyone = (dev_w, dev_p, dev_o, dev_ap, dev_am, dev_bp, dev_bm, dev_s)
    for dev in everyone:
        pl.semaphore_signal(barrier, inc=1, device_id=dev, device_id_type=MESH)

    lane = lax.broadcasted_iota(jnp.int32, (T, 128), 1)
    line = lax.broadcasted_iota(jnp.int32, (T, 128), 0)
    loads[0].wait()

    def rows(start, count):
        return pl.ds(start if isinstance(start, int) else pl.multiple_of(start, count), count)

    def stats(r, carry):
        at = rows(r * T, T)
        v = raw[at, :].astype(F32)
        m = jnp.sum(v, axis=1, keepdims=True) / depth
        d = v - m
        s = jnp.sum(d * d, axis=1, keepdims=True)
        both = jnp.where(lane == line, m, jnp.where(lane == line + T, s, 0.0))
        st_loc[r] = jnp.broadcast_to(jnp.sum(both, axis=0, keepdims=True), (8, 128))
        return carry

    lax.fori_loop(0, 4, stats, 0)
    loads[1].wait()

    pl.semaphore_wait(barrier, len(everyone))

    sends = []

    def remote(src, dst, send, recv, dev, static=True):
        copy = pltpu.make_async_remote_copy(
            src_ref=src, dst_ref=dst, send_sem=send, recv_sem=recv, device_id=dev, device_id_type=MESH
        )
        copy.start()
        if static:
            sends.append(copy)
        return copy

    def arrived(dst, recv, dev):
        pltpu.make_async_remote_copy(
            src_ref=dst, dst_ref=dst, send_sem=recv, recv_sem=recv, device_id=dev, device_id_type=MESH
        ).wait_recv()

    for k, (dev, first, second) in enumerate(((dev_p, z, zp), (dev_w, zo, zw), (dev_o, zw, zo))):
        for h, pos in enumerate((first, second)):
            n = 3 + 2 * k + h
            remote(st_loc.at[pos], st_in.at[k, h], start_send.at[n], start_recv.at[n], dev)
    remote(gain_hbm, gain_other, start_send.at[2], start_recv.at[2], dev_w)
    for k, pos in enumerate((zo, zw)):
        remote(raw.at[rows(pos * T, T)], praw.at[k * T : (k + 1) * T], start_send.at[k], start_recv.at[k], dev_w)

    remote(w_hbm.at[NC * PC :], wG.at[own], w_send.at[NC], w_recv.at[NC], dev_p)

    def send_cols(c):
        remote(w_hbm.at[c * PC : (c + 1) * PC], wP.at[c, own], w_send.at[c], w_recv.at[c], dev_w)

    for c in range(NC - 1):
        send_cols(c)

    def normalise(h, dst, pos):
        for k in range(3):
            n = 3 + 2 * k + h
            arrived(st_in.at[k, h], start_recv.at[n], (dev_p, dev_w, dev_o)[k])
        if h == 0:
            arrived(gain_other, start_recv.at[2], dev_w)
        parts = [st_loc[pos]] + [st_in[k, h] for k in range(3)]
        means = [jnp.sum(jnp.where(lane == line, p[0:1, :], 0.0), axis=1, keepdims=True) for p in parts]
        seconds = [jnp.sum(jnp.where(lane == line + T, p[0:1, :], 0.0), axis=1, keepdims=True) for p in parts]
        mean = (means[0] + means[1] + means[2] + means[3]) * 0.25
        second = jnp.zeros_like(mean)
        for m, v in zip(means, seconds):
            second = second + v + depth * (m - mean) * (m - mean)
        scale = lax.rsqrt(second / width + epsilon)
        dst[own, 0] = ((raw[rows(pos * T, T), :].astype(F32) - mean) * scale * gain[...].reshape(1, depth)).astype(BF16)
        arrived(praw.at[h * T : (h + 1) * T], start_recv.at[h], dev_w)
        dst[other, 0] = (
            (praw[h * T : (h + 1) * T, :].astype(F32) - mean) * scale * gain_other[...].reshape(1, depth)
        ).astype(BF16)

    class Gather:
        def __init__(self, k, buf):
            self.k, self.buf, self.count = k, buf, 0

        def piece(self, i, j, sib=0):
            r = JPOS[j % 4] * 8 + sib * 4 + i % 4
            return self.buf.at[:, r]

        def slot(self, i, s):
            r = i % 4
            return self.buf.at[s, r]

        def rsem(self, i, j, sib=0):
            return g_recv.at[self.k * 32 + sib * 16 + (j % 4) * 4 + i % 4]

        def ssem(self):
            self.count += 1
            return g_send.at[self.k * 36 + self.count - 1]

        def send(self, i, j, di, dj, dev):
            remote(self.piece(i, j), self.piece(i - di, j - dj), self.ssem(), self.rsem(i - di, j - dj), dev)

        def send_sib(self, i, j):
            remote(self.piece(i, j), self.piece(i, j, 1), self.ssem(), self.rsem(i, j, 1), dev_s)

        def send_slot(self, i, di, s, dev):
            remote(self.slot(i, s), self.slot(i - di, s), self.ssem(), g_recv.at[self.k * 32 + (2, 0)[s]], dev)

        def wait(self, i, j, dev, sib=0):
            arrived(self.piece(i, j, sib), self.rsem(i, j, sib), dev)

        def spread(self, i):
            self.send(i, 0, 0, 1, dev_bp)
            self.send(i, 0, 0, -1, dev_bm)
            self.send_sib(i, 0)

        def e1(self):
            self.send(0, 0, 1, 0, dev_ap)
            self.send(0, 0, -1, 0, dev_am)
            self.spread(0)

        def e2(self):
            self.wait(3, 0, dev_am)
            self.send_slot(3, 1, 0, dev_ap)
            self.spread(3)

        def e3(self):
            self.wait(1, 0, dev_ap)
            self.send_slot(1, -1, 1, dev_am)
            self.spread(1)

        def e4(self):
            for s, dev in ((0, dev_am), (1, dev_ap)):
                arrived(self.slot(2, s), g_recv.at[self.k * 32 + (2, 0)[s]], dev)
            self.spread(2)

        def l(self, i):
            self.wait(i, 3, dev_bm)
            if i in (0, 1):
                self.send(i, 3, 0, 1, dev_bp)
            self.send_sib(i, 3)

        def r(self, i):
            self.wait(i, 1, dev_bp)
            if i in (3, 2):
                self.send(i, 1, 0, -1, dev_bm)
            self.send_sib(i, 1)

        def o(self, i):
            self.wait(i, 2, dev_bm if i in (0, 1) else dev_bp)
            self.send_sib(i, 2)

        def e7(self, q):
            j = (0, 1, 3, 2)[q]
            for i in range(4):
                self.wait(i, j, dev_s, 1)

    A, B, C = Gather(0, TA), Gather(1, TB), Gather(2, TC)

    def own_cols(c):
        loads[2 + c].wait()
        arrived(wP.at[c, other], w_recv.at[c], dev_w)

    def by_piece(buf, s, q):
        return buf[s, pl.ds(q * 8, 8)].reshape(QR, depth)

    def by_position(buf, s, q):
        return buf[s, :, rows(q * TR, TR)].reshape(QR, depth)

    def pair_dot(take, buf, c, q):
        return times(take(buf, 0, q), wP[c, 0]) + times(take(buf, 1, q), wP[c, 1])

    def part_copy(n, u):
        return pltpu.make_async_remote_copy(
            src_ref=pbuf.at[n % RING],
            dst_ref=inbuf.at[u],
            send_sem=p_send.at[n],
            recv_sem=p_recv.at[u],
            device_id=dev_p,
            device_id_type=MESH,
        )

    def each(unit, units):
        def step(k, carry):
            u = units[0]
            for n in range(1, len(units)):
                u = jnp.where(k == n, units[n], u)
            unit(k, u)
            return carry

        if len(units) == 1:
            unit(0, units[0])
        else:
            lax.fori_loop(0, len(units), step, 0)

    def runs(units):
        groups = []
        for u in units:
            if groups and (groups[-1][0] < 8) == (u < 8):
                groups[-1].append(u)
            else:
                groups.append([u])
        return groups

    sent = []

    def partial(*units):
        for group in runs(units):
            take = by_piece if group[0] < 8 else by_position
            base = len(sent)

            def unit(k, u):
                n = base + k
                if base >= RING:
                    part_copy(n - RING, u).wait_send()
                pbuf[n % RING] = pair_dot(take, TA, u // 4, u % 4).astype(BF16)
                part_copy(n, u).start()

            if base < RING < base + len(group):
                cut = RING - base
                each(unit, group[:cut])
                sent.extend(group[:cut])
                base = len(sent)
                each(unit, group[cut:])
                sent.extend(group[cut:])
            else:
                each(unit, group)
                sent.extend(group)

    def spot(p):
        pc, px, py = p % 2, (p // 2) % 4, p // 8
        pa = px + pc * (py - px)
        pb = py + pc * (px - py)
        s = (pc + core) % 2
        i = (pa - a + s * (a - b) + 4) % 4
        j = (pb - b + s * (b - a) + 4) % 4
        return (j + (j // 2) * (1 - 2 * (j % 2))) * 8 + s * 4 + i

    spots = [spot(p) for p in range(32)]

    def turn(load, q, start, count):
        for k in range(0, count, 128):
            size = min(128, count - k)
            block = jnp.stack([load(r, k, size) for r in spots])
            at = start + k if isinstance(start, int) else pl.multiple_of(start + k, 128)
            out[rows(q * TR, TR), :, pl.ds(at, size)] = jnp.swapaxes(block, 0, 1).astype(BF16)

    def final(*units):
        for group in runs(units):
            take = by_piece if group[0] < 8 else by_position

            def unit(k, u):
                c, q = u // 4, u % 4
                facc[...] = pair_dot(take, TB, c, q)
                part_copy(u, u).wait_recv()
                total = facc[...] + inbuf[u].astype(F32)
                if take is by_piece:
                    inbuf[u] = total.astype(BF16)
                else:
                    facc[...] = total
                    turn(lambda r, k, n: facc[rows(r * TR, TR), k : k + n], q, c * PC, PC)

            each(unit, group)

    def settle(c):
        def step(q, carry):
            def load(r, k, n):
                return inbuf[c * 4 + r // 8, rows((r % 8) * T + q * TR, TR), k : k + n].astype(F32)

            turn(load, q, c * PC, PC)
            return carry

        lax.fori_loop(0, 4, step, 0)

    def last_a(q):
        at = slice(q * QR, (q + 1) * QR)
        most = times(by_piece(TB, own, q), wF[own]) + times(by_piece(TC, zp % 2, q), wG[zp % 2])
        head = most[:, 0:PC] + times(by_piece(TC, zo % 2, q), wG[zo % 2, 0:PC, :])
        fO[at, 0:PC] = head.astype(BF16)
        fO[at, PC:] = most[:, PC:].astype(BF16)

    def last_b(q, carry):
        at = rows(q * QR, QR)
        fO[at, :] = (fO[at, :].astype(F32) + times(by_piece(TB, other, q), wF[other])).astype(BF16)
        return carry

    def last_c(q, carry):
        facc[:, 0 : fO.shape[1] - PC] = times(by_position(TC, zo % 2, q), wG[zo % 2, PC:, :])

        def load(r, k, n):
            part = fO[rows(r * T + q * TR, TR), k : k + n].astype(F32)
            return part if k < PC else part + facc[rows(r * TR, TR), k - PC : k - PC + n]

        turn(load, q, NC * PC, fO.shape[1])
        return carry

    def forward_last(k):
        part = (slice(0, PC), slice(PC, None))[k]
        remote(wG.at[zp % 2, part], wG.at[zp % 2, part], w_send.at[NC + 2 + k], w_recv.at[NC + 2 + k], dev_w)

    def send_last():
        arrived(wG.at[zp % 2], w_recv.at[NC], dev_p)
        forward_last(0)
        send_cols(NC - 1)
        remote(w_hbm.at[NC * PC :], wF.at[own], w_send.at[NC + 1], w_recv.at[NC + 1], dev_w)
        forward_last(1)

    def send_across():
        remote(A.piece(0, 0), C.piece(0, 0), start_send.at[9], start_recv.at[9], dev_p)

    normalise(0, TA, zp)
    A.e1()
    send_across()
    A.e3()
    A.e2()
    normalise(1, TB, z)
    A.e4()
    A.r(1)
    A.l(1)
    own_cols(0)
    A.l(3)
    A.l(0)
    send_last()
    A.e7(0)
    partial(0)
    B.e1()
    A.l(2)
    A.e7(2)
    A.r(0)
    partial(2)
    A.r(2)
    A.r(3)
    A.e7(1)
    partial(1)
    B.e3()
    A.o(1)
    own_cols(1)
    B.e2()
    partial(6, 4, 5)
    A.o(0)
    A.o(3)
    B.r(1)
    A.o(2)
    arrived(C.piece(0, 0), start_recv.at[9], dev_p)
    B.e4()
    B.r(0)
    B.r(3)
    A.e7(3)
    own_cols(2)
    B.l(0)
    B.l(1)
    partial(10, 9, 7)
    B.l(3)
    B.r(2)
    B.l(2)
    partial(3, 8, 11)
    B.e7(0)
    B.o(0)
    C.e1()
    B.o(3)
    B.e7(1)
    B.e7(2)
    B.o(2)
    B.o(1)
    final(5, 0, 2, 4)
    B.e7(3)
    C.e2()
    C.e3()
    final(6, 10, 7, 1, 9, 3)
    C.e4()
    settle(0)
    C.r(0)
    C.r(3)
    settle(1)
    C.l(1)
    own_cols(3)
    C.e7(0)
    partial(15, 13, 14)
    C.r(1)
    C.l(3)
    C.r(2)
    C.l(2)
    C.l(0)
    final(8, 11)
    partial(12)
    C.o(3)
    C.e7(1)
    loads[2 + NC].wait()
    arrived(wG.at[zo % 2, 0:PC], w_recv.at[NC + 2], dev_w)
    last_a(1)
    C.o(1)
    C.o(0)
    C.o(2)
    C.e7(2)
    last_a(2)
    last_a(0)
    final(15, 13)
    C.e7(3)
    last_a(3)
    arrived(wF.at[other], w_recv.at[NC + 1], dev_w)
    lax.fori_loop(0, 4, last_b, 0)
    final(14)
    arrived(wG.at[zo % 2, PC:], w_recv.at[NC + 3], dev_w)
    lax.fori_loop(0, 4, last_c, 0)
    final(12)

    for copy in sends:
        copy.wait_send()

    def drain(n, carry):
        part_copy(n, n).wait_send()
        return carry

    lax.fori_loop(4 * NC - RING, 4 * NC, drain, 0)


def body(tokens, norm_gain, joined_weight):
    count, depth = tokens.shape
    columns = joined_weight.shape[1]
    rest = columns - NC * PC
    any_space = pl.BlockSpec(memory_space=pl.ANY)
    dma = pltpu.SemaphoreType.DMA
    result = pl.pallas_call(
        kernel,
        out_shape=pltpu.VMEM((T, 32, columns), BF16),
        in_specs=[any_space] * 3,
        out_specs=pl.BlockSpec(memory_space=pltpu.VMEM),
        scratch_shapes=[
            pltpu.VMEM((count, depth), BF16),
            pltpu.VMEM((2 * T, depth), BF16),
            pltpu.VMEM((depth,), F32),
            pltpu.VMEM((depth,), F32),
            pltpu.VMEM((4, 8, 128), F32),
            pltpu.VMEM((3, 2, 8, 128), F32),
            pltpu.VMEM((2, 32, T, depth), BF16),
            pltpu.VMEM((2, 32, T, depth), BF16),
            pltpu.VMEM((2, 32, T, depth), BF16),
            pltpu.VMEM((NC, 2, PC, depth), BF16),
            pltpu.VMEM((2, rest, depth), BF16),
            pltpu.VMEM((2, rest, depth), BF16),
            pltpu.VMEM((RING, QR, PC), BF16),
            pltpu.VMEM((4 * NC, QR, PC), BF16),
            pltpu.VMEM((QR, PC), F32),
            pltpu.VMEM((ROWS, rest), BF16),
            dma((3 + NC,)),
            dma((10,)),
            dma((10,)),
            dma((NC + 4,)),
            dma((NC + 4,)),
            dma((4 * NC,)),
            dma((4 * NC,)),
            dma((3 * 36,)),
            dma((3 * 32,)),
        ],
        compiler_params=pltpu.CompilerParams(
            collective_id=0, has_side_effects=True, vmem_limit_bytes=LIMIT
        ),
    )(tokens, norm_gain, joined_weight.T)
    return result


def solution(mesh):
    return jax.shard_map(
        body,
        mesh=mesh,
        in_specs=(P("gy", "gx"), P("gx"), P("gx", "gy")),
        out_specs=P("gx", None, "gy"),
        check_vma=False,
    )
```

```python
import functools

import jax
import jax.numpy as jnp
from jax import lax
from jax.experimental import pallas as pl
from jax.experimental.pallas import tpu as pltpu
from jax.sharding import PartitionSpec as P

epsilon = 1e-06
MESH = pl.DeviceIdType.MESH
F32 = jnp.float32
BF16 = jnp.bfloat16

PC = 256
NC = 4
T = 64
ROWS = 32 * T
QR = ROWS // 4
TR = T // 4
RING = 7
LIMIT = 61_000_000
JPOS = {0: 0, 1: 1, 3: 2, 2: 3}


def times(rows, columns):
    return lax.dot_general(rows, columns, (((1,), (1,)), ((), ())), preferred_element_type=F32)


def kernel(
    tok_hbm, gain_hbm, w_hbm, out,
    raw, praw, gain, gain_other, st_loc, st_in, TA, TB, TC, wP, wF, wG, pbuf, inbuf, facc, fO,
    lsem, start_send, start_recv, w_send, w_recv, p_send, p_recv, g_send, g_recv,
):
    depth = raw.shape[1]
    width = 4 * depth
    z = lax.axis_index("gx")
    g = lax.axis_index("gy")
    core = g % 2
    x = (g // 2) % 4
    y = g // 8
    a = x + core * (y - x)
    b = y + core * (x - y)

    def gid(a_, b_, core_):
        x_ = a_ + core_ * (b_ - a_)
        y_ = b_ + core_ * (a_ - b_)
        return (y_ * 4 + x_) * 2 + core_

    zw = z + 1 - 2 * (z % 2)
    zp = 3 - z
    zo = (z + 2) % 4
    own = z % 2
    other = 1 - own
    dev_w = (zw, g)
    dev_p = (zp, g)
    dev_o = (zo, g)
    dev_ap = (z, gid((a + 1) % 4, b, core))
    dev_am = (z, gid((a + 3) % 4, b, core))
    dev_bp = (z, gid(a, (b + 1) % 4, core))
    dev_bm = (z, gid(a, (b + 3) % 4, core))
    dev_s = (z, g + 1 - 2 * core)

    loads = [
        pltpu.make_async_copy(tok_hbm, raw, lsem.at[0]),
        pltpu.make_async_copy(gain_hbm, gain, lsem.at[1]),
    ]
    for c in range(NC):
        loads.append(pltpu.make_async_copy(w_hbm.at[c * PC : (c + 1) * PC], wP.at[c, own], lsem.at[2 + c]))
    loads.append(pltpu.make_async_copy(w_hbm.at[NC * PC :], wF.at[own], lsem.at[2 + NC]))
    for copy in loads:
        copy.start()

    barrier = pltpu.get_barrier_semaphore()
    everyone = (dev_w, dev_p, dev_o, dev_ap, dev_am, dev_bp, dev_bm, dev_s)
    for dev in everyone:
        pl.semaphore_signal(barrier, inc=1, device_id=dev, device_id_type=MESH)

    lane = lax.broadcasted_iota(jnp.int32, (T, 128), 1)
    line = lax.broadcasted_iota(jnp.int32, (T, 128), 0)
    loads[0].wait()

    def rows(start, count):
        return pl.ds(start if isinstance(start, int) else pl.multiple_of(start, count), count)

    def stats(r, carry):
        at = rows(r * T, T)
        v = raw[at, :].astype(F32)
        m = jnp.sum(v, axis=1, keepdims=True) / depth
        d = v - m
        s = jnp.sum(d * d, axis=1, keepdims=True)
        both = jnp.where(lane == line, m, jnp.where(lane == line + T, s, 0.0))
        st_loc[r] = jnp.broadcast_to(jnp.sum(both, axis=0, keepdims=True), (8, 128))
        return carry

    lax.fori_loop(0, 4, stats, 0)
    loads[1].wait()

    pl.semaphore_wait(barrier, len(everyone))

    sends = []

    def remote(src, dst, send, recv, dev, static=True):
        copy = pltpu.make_async_remote_copy(
            src_ref=src, dst_ref=dst, send_sem=send, recv_sem=recv, device_id=dev, device_id_type=MESH
        )
        copy.start()
        if static:
            sends.append(copy)
        return copy

    def arrived(dst, recv, dev):
        pltpu.make_async_remote_copy(
            src_ref=dst, dst_ref=dst, send_sem=recv, recv_sem=recv, device_id=dev, device_id_type=MESH
        ).wait_recv()

    for k, (dev, first, second) in enumerate(((dev_p, z, zp), (dev_w, zo, zw), (dev_o, zw, zo))):
        for h, pos in enumerate((first, second)):
            n = 3 + 2 * k + h
            remote(st_loc.at[pos], st_in.at[k, h], start_send.at[n], start_recv.at[n], dev)
    remote(gain_hbm, gain_other, start_send.at[2], start_recv.at[2], dev_w)
    for k, pos in enumerate((zo, zw)):
        remote(raw.at[rows(pos * T, T)], praw.at[k * T : (k + 1) * T], start_send.at[k], start_recv.at[k], dev_w)

    remote(w_hbm.at[NC * PC :], wG.at[own], w_send.at[NC], w_recv.at[NC], dev_p)

    def send_cols(c):
        remote(w_hbm.at[c * PC : (c + 1) * PC], wP.at[c, own], w_send.at[c], w_recv.at[c], dev_w)

    for c in range(NC - 1):
        send_cols(c)

    def normalise(h, dst, pos):
        for k in range(3):
            n = 3 + 2 * k + h
            arrived(st_in.at[k, h], start_recv.at[n], (dev_p, dev_w, dev_o)[k])
        if h == 0:
            arrived(gain_other, start_recv.at[2], dev_w)
        parts = [st_loc[pos]] + [st_in[k, h] for k in range(3)]
        means = [jnp.sum(jnp.where(lane == line, p[0:1, :], 0.0), axis=1, keepdims=True) for p in parts]
        seconds = [jnp.sum(jnp.where(lane == line + T, p[0:1, :], 0.0), axis=1, keepdims=True) for p in parts]
        mean = (means[0] + means[1] + means[2] + means[3]) * 0.25
        second = jnp.zeros_like(mean)
        for m, v in zip(means, seconds):
            second = second + v + depth * (m - mean) * (m - mean)
        scale = lax.rsqrt(second / width + epsilon)
        dst[own, 0] = ((raw[rows(pos * T, T), :].astype(F32) - mean) * scale * gain[...].reshape(1, depth)).astype(BF16)
        arrived(praw.at[h * T : (h + 1) * T], start_recv.at[h], dev_w)
        dst[other, 0] = (
            (praw[h * T : (h + 1) * T, :].astype(F32) - mean) * scale * gain_other[...].reshape(1, depth)
        ).astype(BF16)

    class Gather:
        def __init__(self, k, buf):
            self.k, self.buf, self.count = k, buf, 0

        def piece(self, i, j, sib=0):
            r = JPOS[j % 4] * 8 + sib * 4 + i % 4
            return self.buf.at[:, r]

        def slot(self, i, s):
            r = i % 4
            return self.buf.at[s, r]

        def rsem(self, i, j, sib=0):
            return g_recv.at[self.k * 32 + sib * 16 + (j % 4) * 4 + i % 4]

        def ssem(self):
            self.count += 1
            return g_send.at[self.k * 36 + self.count - 1]

        def send(self, i, j, di, dj, dev):
            remote(self.piece(i, j), self.piece(i - di, j - dj), self.ssem(), self.rsem(i - di, j - dj), dev)

        def send_sib(self, i, j):
            remote(self.piece(i, j), self.piece(i, j, 1), self.ssem(), self.rsem(i, j, 1), dev_s)

        def send_slot(self, i, di, s, dev):
            remote(self.slot(i, s), self.slot(i - di, s), self.ssem(), g_recv.at[self.k * 32 + (2, 0)[s]], dev)

        def wait(self, i, j, dev, sib=0):
            arrived(self.piece(i, j, sib), self.rsem(i, j, sib), dev)

        def spread(self, i):
            self.send(i, 0, 0, 1, dev_bp)
            self.send(i, 0, 0, -1, dev_bm)
            self.send_sib(i, 0)

        def e1(self):
            self.send(0, 0, 1, 0, dev_ap)
            self.send(0, 0, -1, 0, dev_am)
            self.spread(0)

        def e2(self):
            self.wait(3, 0, dev_am)
            self.send_slot(3, 1, 0, dev_ap)
            self.spread(3)

        def e3(self):
            self.wait(1, 0, dev_ap)
            self.send_slot(1, -1, 1, dev_am)
            self.spread(1)

        def e4(self):
            for s, dev in ((0, dev_am), (1, dev_ap)):
                arrived(self.slot(2, s), g_recv.at[self.k * 32 + (2, 0)[s]], dev)
            self.spread(2)

        def l(self, i):
            self.wait(i, 3, dev_bm)
            if i in (0, 1):
                self.send(i, 3, 0, 1, dev_bp)
            self.send_sib(i, 3)

        def r(self, i):
            self.wait(i, 1, dev_bp)
            if i in (3, 2):
                self.send(i, 1, 0, -1, dev_bm)
            self.send_sib(i, 1)

        def o(self, i):
            self.wait(i, 2, dev_bm if i in (0, 1) else dev_bp)
            self.send_sib(i, 2)

        def e7(self, q):
            j = (0, 1, 3, 2)[q]
            for i in range(4):
                self.wait(i, j, dev_s, 1)

    A, B, C = Gather(0, TA), Gather(1, TB), Gather(2, TC)

    def own_cols(c):
        loads[2 + c].wait()
        arrived(wP.at[c, other], w_recv.at[c], dev_w)

    def by_piece(buf, s, q):
        return buf[s, pl.ds(q * 8, 8)].reshape(QR, depth)

    def by_position(buf, s, q):
        return buf[s, :, rows(q * TR, TR)].reshape(QR, depth)

    def pair_dot(take, buf, c, q):
        return times(take(buf, 0, q), wP[c, 0]) + times(take(buf, 1, q), wP[c, 1])

    def part_copy(n, u):
        return pltpu.make_async_remote_copy(
            src_ref=pbuf.at[n % RING],
            dst_ref=inbuf.at[u],
            send_sem=p_send.at[n],
            recv_sem=p_recv.at[u],
            device_id=dev_p,
            device_id_type=MESH,
        )

    def each(unit, units):
        def step(k, carry):
            u = units[0]
            for n in range(1, len(units)):
                u = jnp.where(k == n, units[n], u)
            unit(k, u)
            return carry

        if len(units) == 1:
            unit(0, units[0])
        else:
            lax.fori_loop(0, len(units), step, 0)

    def runs(units):
        groups = []
        for u in units:
            if groups and (groups[-1][0] < 8) == (u < 8):
                groups[-1].append(u)
            else:
                groups.append([u])
        return groups

    sent = []

    def partial(*units):
        for group in runs(units):
            take = by_piece if group[0] < 8 else by_position
            base = len(sent)

            def unit(k, u):
                n = base + k
                if base >= RING:
                    part_copy(n - RING, u).wait_send()
                pbuf[n % RING] = pair_dot(take, TA, u // 4, u % 4).astype(BF16)
                part_copy(n, u).start()

            if base < RING < base + len(group):
                cut = RING - base
                each(unit, group[:cut])
                sent.extend(group[:cut])
                base = len(sent)
                each(unit, group[cut:])
                sent.extend(group[cut:])
            else:
                each(unit, group)
                sent.extend(group)

    def spot(p):
        pc, px, py = p % 2, (p // 2) % 4, p // 8
        pa = px + pc * (py - px)
        pb = py + pc * (px - py)
        s = (pc + core) % 2
        i = (pa - a + s * (a - b) + 4) % 4
        j = (pb - b + s * (b - a) + 4) % 4
        return (j + (j // 2) * (1 - 2 * (j % 2))) * 8 + s * 4 + i

    spots = [spot(p) for p in range(32)]

    def turn(load, q, start, count):
        for k in range(0, count, 128):
            size = min(128, count - k)
            block = jnp.stack([load(r, k, size) for r in spots])
            at = start + k if isinstance(start, int) else pl.multiple_of(start + k, 128)
            out[rows(q * TR, TR), :, pl.ds(at, size)] = jnp.swapaxes(block, 0, 1).astype(BF16)

    def final(*units):
        for group in runs(units):
            take = by_piece if group[0] < 8 else by_position

            def unit(k, u):
                c, q = u // 4, u % 4
                facc[...] = pair_dot(take, TB, c, q)
                part_copy(u, u).wait_recv()
                total = facc[...] + inbuf[u].astype(F32)
                if take is by_piece:
                    inbuf[u] = total.astype(BF16)
                else:
                    facc[...] = total
                    turn(lambda r, k, n: facc[rows(r * TR, TR), k : k + n], q, c * PC, PC)

            each(unit, group)

    def settle(c):
        def step(q, carry):
            def load(r, k, n):
                return inbuf[c * 4 + r // 8, rows((r % 8) * T + q * TR, TR), k : k + n].astype(F32)

            turn(load, q, c * PC, PC)
            return carry

        lax.fori_loop(0, 4, step, 0)

    def last_a(q):
        at = slice(q * QR, (q + 1) * QR)
        most = times(by_piece(TB, own, q), wF[own]) + times(by_piece(TC, zp % 2, q), wG[zp % 2])
        head = most[:, 0:PC] + times(by_piece(TC, zo % 2, q), wG[zo % 2, 0:PC, :])
        fO[at, 0:PC] = head.astype(BF16)
        fO[at, PC:] = most[:, PC:].astype(BF16)

    def last_b(q, carry):
        at = rows(q * QR, QR)
        fO[at, :] = (fO[at, :].astype(F32) + times(by_piece(TB, other, q), wF[other])).astype(BF16)
        return carry

    def last_c(q, carry):
        facc[:, 0 : fO.shape[1] - PC] = times(by_position(TC, zo % 2, q), wG[zo % 2, PC:, :])

        def load(r, k, n):
            part = fO[rows(r * T + q * TR, TR), k : k + n].astype(F32)
            return part if k < PC else part + facc[rows(r * TR, TR), k - PC : k - PC + n]

        turn(load, q, NC * PC, fO.shape[1])
        return carry

    def forward_last(k):
        part = (slice(0, PC), slice(PC, None))[k]
        remote(wG.at[zp % 2, part], wG.at[zp % 2, part], w_send.at[NC + 2 + k], w_recv.at[NC + 2 + k], dev_w)

    def send_last():
        arrived(wG.at[zp % 2], w_recv.at[NC], dev_p)
        forward_last(0)
        send_cols(NC - 1)
        remote(w_hbm.at[NC * PC :], wF.at[own], w_send.at[NC + 1], w_recv.at[NC + 1], dev_w)
        forward_last(1)

    def send_across():
        remote(A.piece(0, 0), C.piece(0, 0), start_send.at[9], start_recv.at[9], dev_p)

    normalise(0, TA, zp)
    A.e1()
    A.e2()
    A.e3()
    A.e4()
    send_across()
    normalise(1, TB, z)
    A.l(3)
    A.r(0)
    A.l(0)
    own_cols(0)
    A.e7(0)
    A.r(3)
    A.r(1)
    A.l(1)
    partial(0)
    A.r(2)
    A.l(2)
    A.e7(1)
    B.e1()
    A.e7(2)
    partial(2, 1)
    own_cols(1)
    A.o(1)
    A.o(3)
    send_last()
    A.o(2)
    A.o(0)
    B.e2()
    partial(4, 6, 5)
    B.e3()
    B.e4()
    B.l(0)
    B.r(0)
    arrived(C.piece(0, 0), start_recv.at[9], dev_p)
    B.l(3)
    B.r(3)
    B.e7(0)
    own_cols(2)
    A.e7(3)
    B.l(1)
    B.r(1)
    C.e1()
    partial(10, 7, 3)
    B.l(2)
    final(4, 0)
    B.r(2)
    B.e7(1)
    C.e2()
    C.e3()
    final(1, 5)
    partial(8)
    B.o(3)
    partial(11)
    B.o(1)
    C.e4()
    C.r(0)
    B.e7(2)
    loads[2 + NC].wait()
    arrived(wG.at[zo % 2, 0:PC], w_recv.at[NC + 2], dev_w)
    B.o(0)
    final(2, 6)
    C.e7(0)
    B.o(2)
    partial(9)
    last_a(0)
    B.e7(3)
    C.l(0)
    C.l(3)
    C.r(3)
    final(10, 7, 8, 3)
    C.r(1)
    own_cols(3)
    settle(0)
    settle(1)
    C.r(2)
    C.l(1)
    partial(15, 13, 12)
    C.l(2)
    C.o(3)
    partial(14)
    C.o(0)
    final(9, 11)
    C.o(2)
    C.o(1)
    C.e7(2)
    C.e7(1)
    last_a(1)
    final(15)
    C.e7(3)
    last_a(3)
    last_a(2)
    final(13)
    arrived(wF.at[other], w_recv.at[NC + 1], dev_w)
    lax.fori_loop(0, 4, last_b, 0)
    final(12)
    arrived(wG.at[zo % 2, PC:], w_recv.at[NC + 3], dev_w)
    lax.fori_loop(0, 4, last_c, 0)
    final(14)

    for copy in sends:
        copy.wait_send()

    def drain(n, carry):
        part_copy(n, n).wait_send()
        return carry

    lax.fori_loop(4 * NC - RING, 4 * NC, drain, 0)


def body(tokens, norm_gain, joined_weight):
    count, depth = tokens.shape
    columns = joined_weight.shape[1]
    rest = columns - NC * PC
    any_space = pl.BlockSpec(memory_space=pl.ANY)
    dma = pltpu.SemaphoreType.DMA
    result = pl.pallas_call(
        kernel,
        out_shape=pltpu.VMEM((T, 32, columns), BF16),
        in_specs=[any_space] * 3,
        out_specs=pl.BlockSpec(memory_space=pltpu.VMEM),
        scratch_shapes=[
            pltpu.VMEM((count, depth), BF16),
            pltpu.VMEM((2 * T, depth), BF16),
            pltpu.VMEM((depth,), F32),
            pltpu.VMEM((depth,), F32),
            pltpu.VMEM((4, 8, 128), F32),
            pltpu.VMEM((3, 2, 8, 128), F32),
            pltpu.VMEM((2, 32, T, depth), BF16),
            pltpu.VMEM((2, 32, T, depth), BF16),
            pltpu.VMEM((2, 32, T, depth), BF16),
            pltpu.VMEM((NC, 2, PC, depth), BF16),
            pltpu.VMEM((2, rest, depth), BF16),
            pltpu.VMEM((2, rest, depth), BF16),
            pltpu.VMEM((RING, QR, PC), BF16),
            pltpu.VMEM((4 * NC, QR, PC), BF16),
            pltpu.VMEM((QR, PC), F32),
            pltpu.VMEM((ROWS, rest), BF16),
            dma((3 + NC,)),
            dma((10,)),
            dma((10,)),
            dma((NC + 4,)),
            dma((NC + 4,)),
            dma((4 * NC,)),
            dma((4 * NC,)),
            dma((3 * 36,)),
            dma((3 * 32,)),
        ],
        compiler_params=pltpu.CompilerParams(
            collective_id=0, has_side_effects=True, vmem_limit_bytes=LIMIT
        ),
    )(tokens, norm_gain, joined_weight.T)
    return result


def solution(mesh):
    return jax.shard_map(
        body,
        mesh=mesh,
        in_specs=(P("gy", "gx"), P("gx"), P("gx", "gy")),
        out_specs=P("gx", None, "gy"),
        check_vma=False,
    )
```
